32 devices in a mesh: gx: 4 (over x, core), gy: 2 (over y), gz: 4 (over z).
Axes of the slice: x: 2, y: 2, z: 4, core: 2. Of those that a mesh axis runs over, the one named last changes fastest.
Arguments:
- tokens: bfloat16 [1024, 6144], P('gy', ('gz', 'gx')), may hold values from -6 to 6
- weight: bfloat16 [6144, 24576], P('gz', ('gx', 'gy')), may hold values from -0.109375 to 0.109375
- bias: float32 [24576], P(('gx', 'gz')), may hold values from -4 to 4
Outputs:
- hidden: bfloat16 [1024, 24576], P('gy', ('gx', 'gz'))
The draws below stay inside these ranges and needn't reach their ends.
All inputs are finite; a program needn't handle non-finite values.
Results may differ from the reference program's by a relative error of at most 0.001.
Values may be sent and summed in bfloat16 or wider, within the bound.
A program may use at most 128 MiB of HBM per device.

```python
import jax
import jax.numpy as jnp

D = 6144
FF = 24576
TOKENS = 1024


def spiked(values, rng, source, target, shards_of, factor):
    owner, partner = [(jnp.arange(values.shape[axis_at]) // (values.shape[axis_at] // shards_of)).reshape([-1 if axis == axis_at else 1 for axis in range(values.ndim)]) for axis_at in (source, target)]
    chosen = jax.random.permutation(rng, shards_of)[partner]
    strong = (owner == chosen) | (owner == (partner + shards_of // 2) % shards_of)
    return jnp.where(strong, factor * values, values)


def level_of(key, dims, split, least, high):
    level = 1.0
    for position, shards_of in split:
        heights = jax.random.uniform(jax.random.fold_in(jax.random.fold_in(key, 6), position), (shards_of,), jnp.float32, least / len(split), high / len(split))
        level = level * jnp.repeat(jnp.exp(heights), dims[position] // shards_of).reshape((-1,) + (1,) * (len(dims) - 1 - position))
    return level


def scatter_about(key, extent, width, limit, shards=(), held_as=jnp.bfloat16):
    drawn = width * jax.random.normal(key, extent, jnp.float32)
    if shards:
        drawn = drawn * level_of(key, extent, shards, -0.22, 0.18)
    return jnp.clip(drawn, -limit, limit).astype(held_as)


def heavy_noise(stream_key, shape, spread, limit, cuts, heavy, kind=jnp.bfloat16):
    array = spread * jax.random.normal(stream_key, shape, jnp.float32)
    if cuts:
        array = array * level_of(stream_key, shape, cuts, -0.22, 0.18)
    return jnp.clip(spiked(array, jax.random.fold_in(stream_key, 3), *heavy), -limit, limit).astype(kind)


def setup_inputs(seed: int = 0) -> dict:
    key_list = jax.random.split(jax.random.key(seed), 4)
    return {
        "tokens": scatter_about(key_list[0], (TOKENS, D), 1.0, 6.0, ((0, 2), (1, 16))),
        "weight": heavy_noise(key_list[1], (D, FF), D ** -0.5, 0.109375, ((0, 4), (1, 8)), (0, 1, 8, 2.0)),
        "bias": scatter_about(key_list[2], (FF,), 1.0, 4.0, ((0, 16),), jnp.float32),
    }


def reference(tokens, weight, bias):
    pre = jnp.dot(tokens, weight, preferred_element_type=jnp.float32) + bias.astype(jnp.float32)
    return jax.nn.gelu(pre, approximate=False).astype(jnp.bfloat16)
```

```python
import functools

import jax
import jax.numpy as jnp
from jax import lax
from jax.experimental import pallas as pl
from jax.experimental.pallas import tpu as pltpu
from jax.sharding import PartitionSpec as P

MESH = pl.DeviceIdType.MESH
POWER = 11


def encode(p):
    p2 = p * p
    p4 = p2 * p2
    return ((p4 * p4) * (p2 * p)).astype(jnp.bfloat16)


def decode(code):
    y = code.astype(jnp.float32)
    a = jnp.maximum(jnp.abs(y), 1e-37)
    scale = -(POWER - 1) / POWER * 1.4426950408889634
    return y * jnp.exp2(jnp.log(a) * scale)


def gelu(v):
    return (v * 0.5) * (1.0 + lax.erf(v * 0.7071067811865476))


def kernel(nb, hr, cw, pieces, tok, w, bias, out, t, wv, acc, ysend, yrecv, zsend, ra, rb,
           ws, os, ts, tr, yss, yrs, zss, ras, rbs):
    gx, y, z = (lax.axis_index(a) for a in ("gx", "gy", "gz"))
    fdim = tok.shape[1]
    nc = 2 * nb
    core = gx + 1 - 2 * lax.rem(gx, 2)
    xp = lax.rem(gx + 2, 4)
    oy = 1 - y
    end = (z == 0) | (z == 3)
    middle = jnp.logical_not(end)
    low = z < 2
    own_half = y == z // 2
    other_half = jnp.logical_not(own_half)
    inner = jnp.where(low, 1, 2)
    far_mid = jnp.where(low, 2, 1)
    near = jnp.where(low, 0, 3)
    one = jnp.where(low, 1, 0)
    zero = 1 - one
    first = jnp.where(end, one, y)

    def wcopy(k):
        cols = pl.ds(pl.multiple_of(k * cw, cw), cw)
        return pltpu.make_async_copy(w.at[:, cols], wv.at[k], ws.at[k])

    def slot(r, g, q):
        lo, n = pieces[q]
        return t.at[r, pl.ds(lo, n), pl.ds(pl.multiple_of(g * fdim, 128), fdim)]

    own_tok = pltpu.make_async_copy(
        tok, t.at[y, :, pl.ds(pl.multiple_of(gx * fdim, 128), fdim)], os.at[0])
    own_tok.start()
    lead = jnp.where(own_half, one, jnp.where(end, one, 0))

    def wstart(k, carry):
        wcopy(lax.rem(k + lead * nb, nc)).start()
        return carry

    lax.fori_loop(0, nc, wstart, 0)

    barrier = pltpu.get_barrier_semaphore()

    def hello(dev):
        pl.semaphore_signal(barrier, inc=1, device_id=dev, device_id_type=MESH)

    hello((core, y, z))
    hello((xp, y, z))
    hello((gx, oy, z))

    @pl.when(z > 0)
    def _():
        hello((gx, y, z - 1))

    @pl.when(z < 3)
    def _():
        hello((gx, y, z + 1))

    own_tok.wait()
    pl.semaphore_wait(barrier, jnp.where(end, 4, 5))

    def send(k, q, ref, dev):
        return pltpu.make_async_remote_copy(
            src_ref=ref, dst_ref=ref, send_sem=ts.at[k, q], recv_sem=tr.at[k, q],
            device_id=dev, device_id_type=MESH)

    to_core, to_x, to_y = (core, y, z), (xp, y, z), (gx, oy, z)
    nq = len(pieces)
    c0 = [send(0, q, slot(y, gx, q), to_core) for q in range(nq)]
    c1 = [send(1, q, slot(y, gx, q), to_x) for q in range(nq)]
    c2 = [send(2, q, slot(y, gx, q), to_y) for q in range(nq)]
    c3 = [send(3, q, slot(y, xp, q), to_core) for q in range(nq)]
    c4 = [send(4, q, slot(oy, gx, q), to_core) for q in range(nq)]
    c5 = [send(5, q, slot(oy, gx, q), to_x) for q in range(nq)]
    c6 = [send(6, q, slot(oy, xp, q), to_core) for q in range(nq)]
    for q in range(nq):
        c1[q].start()
        c0[q].start()
        c2[q].start()

    def own_rows(q):
        c1[q].wait_recv()
        c3[q].start()
        c0[q].wait_recv()
        c3[q].wait_recv()

    def pass_on(q):
        c2[q].wait_recv()
        c5[q].start()
        c4[q].start()

    def other_rows(q):
        c5[q].wait_recv()
        c6[q].start()
        c4[q].wait_recv()
        c6[q].wait_recv()

    def split(c):
        return lax.div(c, nb), lax.rem(c, nb)

    def dot(r, j, c):
        h, b = split(c)
        rows = pl.ds(pl.multiple_of(h * hr, hr), hr)
        return jnp.dot(t[r, rows], wv[j * nb + b], preferred_element_type=jnp.float32)

    def ycopy(j, c):
        return pltpu.make_async_remote_copy(
            src_ref=ysend.at[j, c], dst_ref=yrecv.at[j, c], send_sem=yss.at[j, c],
            recv_sem=yrs.at[j, c], device_id=(gx, oy, z), device_id_type=MESH)

    def zcopy(src, k, c, dst, sem, m, dev):
        return pltpu.make_async_remote_copy(
            src_ref=src.at[k[0], c], dst_ref=dst.at[m, c], send_sem=zss.at[k[1], c],
            recv_sem=sem.at[m, c], device_id=(gx, y, dev), device_id_type=MESH)

    def from_end(m, c):
        return zcopy(zsend, (m, m), c, ra, ras, m, inner)

    def from_mid(m, c):
        return zcopy(zsend, (m, m), c, rb, rbs, m, far_mid)

    def loop(lo, hi, body):
        def run(c, carry):
            body(c)
            return carry
        lax.fori_loop(lo, hi, run, 0)

    def give(j, c):
        ysend[j, c] = encode(dot(oy, j, c))
        ycopy(j, c).start()

    def finish(c, value):
        h, b = split(c)
        rows = pl.ds(pl.multiple_of(h * hr, hr), hr)
        cols = pl.ds(pl.multiple_of(b * cw, cw), cw)
        out[rows, cols] = gelu(value + bias[:, cols]).astype(out.dtype)

    loop(0, nc, lambda k: wcopy(k).wait())

    def end_send(s, j, c):
        zsend[s, c] = encode(dot(y, j, c))
        from_end(s, c).start()

    def relay(s, j, c):
        ycopy(j, c).wait_recv()
        zcopy(yrecv, (j, s), c, ra, ras, s, inner).start()

    def end_last(own, c):
        if own:
            acc[...] = dot(y, zero, c)
        else:
            ycopy(zero, c).wait_recv()
            acc[...] = decode(yrecv[zero, c])
        zcopy(zsend, (0, 0), c, rb, rbs, 1, z).wait_recv()
        finish(c, acc[...] + decode(rb[1, c]))

    early = 2
    early_rows = [q for q in range(nq) if pieces[q][0] + pieces[q][1] <= hr]
    late_rows = [q for q in range(nq) if q not in early_rows]

    def opening(s):
        for q in early_rows:
            own_rows(q)
            lo, n = pieces[q]
            rows = pl.ds(lo, n)
            for b in range(early):
                zsend[s, b, rows] = encode(jnp.dot(
                    t[y, rows], wv[one * nb + b], preferred_element_type=jnp.float32))
                pltpu.make_async_remote_copy(
                    src_ref=zsend.at[s, b, rows], dst_ref=ra.at[s, b, rows],
                    send_sem=zss.at[s, b], recv_sem=ras.at[s, b],
                    device_id=(gx, y, inner), device_id_type=MESH).start()
            pass_on(q)
        loop(early, nb, lambda c: end_send(s, one, c))
        for q in late_rows:
            own_rows(q)
            pass_on(q)

    ahead = (2 * nc) // 3

    @pl.when(end & own_half)
    def _():
        opening(2)
        loop(nb, ahead, lambda c: end_send(2, one, c))
        for q in early_rows:
            other_rows(q)
        loop(0, nb, lambda c: give(one, c))
        for q in late_rows:
            other_rows(q)
        loop(nb, nc, lambda c: give(one, c))

        def far(c):
            relay(0, one, c)
            give(zero, c)

        loop(0, nc, far)
        loop(0, nc, lambda c: relay(1, zero, c))
        loop(ahead, nc, lambda c: end_send(2, one, c))
        loop(0, nc, lambda c: end_last(True, c))

    @pl.when(end & other_half)
    def _():
        opening(0)
        loop(nb, nc, lambda c: end_send(0, one, c))
        for q in early_rows:
            other_rows(q)
        loop(0, nb, lambda c: give(one, c))
        for q in late_rows:
            other_rows(q)
        loop(nb, nc, lambda c: give(one, c))
        loop(0, nc, lambda c: give(zero, c))
        loop(0, nc, lambda c: end_send(1, zero, c))
        loop(0, nc, lambda c: relay(2, one, c))
        loop(0, nc, lambda c: end_last(False, c))

    def partial_of(own, j, c):
        if own:
            return dot(y, j, c)
        ycopy(j, c).wait_recv()
        return decode(yrecv[j, c])

    def up(own, s, j, c):
        acc[...] = partial_of(own, j, c)
        zcopy(zsend, (s, s), c, ra, ras, s, z).wait_recv()
        zsend[s, c] = encode(acc[...] + decode(ra[s, c]))
        from_mid(s, c).start()

    def down(own, j, c):
        acc[...] = partial_of(own, j, c)
        zcopy(zsend, (2, 2), c, rb, rbs, 0, z).wait_recv()
        zsend[2, c] = encode(acc[...] + decode(rb[0, c]))
        zcopy(zsend, (2, 2), c, rb, rbs, 1, near).start()

    def mid_last(own, j, c):
        part = partial_of(own, j, c)
        zcopy(zsend, (0, 0), c, rb, rbs, 1, z).wait_recv()
        acc[...] = part + decode(rb[1, c])
        zcopy(zsend, (0, 0), c, ra, ras, 2, z).wait_recv()
        finish(c, acc[...] + decode(ra[2, c]))

    @pl.when(middle)
    def _():
        for q in range(nq):
            own_rows(q)
            pass_on(q)
        for q in early_rows:
            other_rows(q)
        loop(0, nb, lambda c: give(first, c))
        for q in late_rows:
            other_rows(q)
        loop(nb, nc, lambda c: give(first, c))
        loop(0, nc, lambda c: give(1 - first, c))

    lag = nb

    @pl.when(middle & own_half)
    def _():
        loop(0, lag, lambda c: down(True, zero, c))

        def both(c):
            up(False, 0, one, c)
            down(True, zero, c + lag)

        loop(0, nc - lag, both)
        loop(nc - lag, nc, lambda c: up(False, 0, one, c))

        def mixed(c):
            up(False, 1, zero, c)
            mid_last(True, one, c)

        loop(0, ahead, mixed)
        loop(ahead, nc, lambda c: up(False, 1, zero, c))
        loop(ahead, nc, lambda c: mid_last(True, one, c))

    @pl.when(middle & other_half)
    def _():
        loop(0, nc, lambda c: up(True, 0, one, c))

        def both(c):
            up(True, 1, zero, c)
            down(False, zero, c)

        loop(0, nc, both)
        loop(0, nc, lambda c: mid_last(False, one, c))

    for group in (c0, c1, c2, c3, c4, c5, c6):
        for c in group:
            c.wait_send()

    def drain(c):
        for s in range(3):
            from_end(s, c).wait_send()
        for j in range(2):
            ycopy(j, c).wait_send()

    loop(0, nc, drain)


def fused(tokens, weight, bias):
    rows, fdim = tokens.shape
    depth, cols = weight.shape
    block = cols // 2
    cw = 256
    hr = rows // 2
    nb = block // cw
    nc = 2 * nb
    pieces = ((0, rows // 8), (rows // 8, rows // 8), (rows // 4, rows // 4), (hr, hr))
    nq = len(pieces)
    dma = pltpu.SemaphoreType.DMA
    piece = lambda n: pltpu.VMEM((n, nc, hr, cw), jnp.bfloat16)
    return pl.pallas_call(
        functools.partial(kernel, nb, hr, cw, pieces),
        out_shape=jax.ShapeDtypeStruct((rows, block), jnp.bfloat16),
        in_specs=[
            pl.BlockSpec(memory_space=pltpu.HBM),
            pl.BlockSpec(memory_space=pltpu.HBM),
            pl.BlockSpec(memory_space=pltpu.VMEM),
        ],
        out_specs=pl.BlockSpec(memory_space=pltpu.VMEM),
        scratch_shapes=[
            pltpu.VMEM((2, rows, depth), jnp.bfloat16),
            pltpu.VMEM((nc, depth, cw), jnp.bfloat16),
            pltpu.VMEM((hr, cw), jnp.float32),
            piece(2), piece(2), piece(3), piece(3), piece(2),
            dma((nc,)), dma((1,)), dma((7, nq)), dma((7, nq)), dma((2, nc)), dma((2, nc)),
            dma((3, nc)), dma((3, nc)), dma((2, nc)),
        ],
        compiler_params=pltpu.CompilerParams(
            has_side_effects=True, collective_id=0, vmem_limit_bytes=60 * 1024 * 1024),
    )(tokens, weight, bias[None, :])


def gathered(tokens, weight, bias):
    features = lax.all_gather(tokens, "gx", axis=1, tiled=True)
    columns = lax.all_gather(weight, "gy", axis=1, tiled=True)
    partial_sum = jnp.dot(features, columns, preferred_element_type=jnp.float32)
    owned = lax.psum_scatter(partial_sum, "gz", scatter_dimension=1, tiled=True)
    pre = owned + bias[None, :]
    return jax.nn.gelu(pre, approximate=False).astype(jnp.bfloat16)


def solution(mesh):
    placed = (P("gy", ("gz", "gx")), P("gz", ("gx", "gy")), P(("gx", "gz")))
    sizes = tuple(mesh.shape[a] for a in ("gx", "gy", "gz"))
    per_device = fused if sizes == (4, 2, 4) else gathered
    return jax.shard_map(
        per_device, mesh=mesh, in_specs=placed, out_specs=P("gy", ("gx", "gz")), check_vma=False
    )
```

```python
import functools

import jax
import jax.numpy as jnp
from jax import lax
from jax.experimental import pallas as pl
from jax.experimental.pallas import tpu as pltpu
from jax.sharding import PartitionSpec as P

MESH = pl.DeviceIdType.MESH
POWER = 11


def encode(p):
    p2 = p * p
    p4 = p2 * p2
    return ((p4 * p4) * (p2 * p)).astype(jnp.bfloat16)


def decode(code):
    y = code.astype(jnp.float32)
    a = jnp.maximum(jnp.abs(y), 1e-37)
    scale = -(POWER - 1) / POWER * 1.4426950408889634
    return y * jnp.exp2(jnp.log(a) * scale)


def gelu(v):
    return (v * 0.5) * (1.0 + lax.erf(v * 0.7071067811865476))


def kernel(nb, hr, cw, group, pieces, tok, w, bias, out, t, wv, bv, acc, ysend, yrecv,
           zsend, ra, rb, ws, os, ts, r0, r1, r2, r3, r4, yss, yrs, zss, ras, rms, rbs):
    gx, y, z = (lax.axis_index(a) for a in ("gx", "gy", "gz"))
    rows_all, fdim = tok.shape
    nc = 2 * nb
    core = gx + 1 - 2 * lax.rem(gx, 2)
    xp = lax.rem(gx + 2, 4)
    xq = lax.rem(core + 2, 4)
    oy = 1 - y
    end = (z == 0) | (z == 3)
    middle = jnp.logical_not(end)
    low = z < 2
    own_half = y == z // 2
    other_half = jnp.logical_not(own_half)
    inner = jnp.where(low, 1, 2)
    far_mid = jnp.where(low, 2, 1)
    near = jnp.where(low, 0, 3)
    one = jnp.where(low, 1, 0)
    zero = 1 - one
    first = jnp.where(end, one, y)

    def loop(lo, hi, body):
        def run(c, carry):
            body(c)
            return carry
        lax.fori_loop(lo, hi, run, 0)

    half = nb // 2

    def wcopy(k):
        cols = pl.ds(pl.multiple_of(k * 2 * cw, 2 * cw), 2 * cw)
        return pltpu.make_async_copy(w.at[:, cols], wv.at[k], ws.at[k])

    def feats(g):
        return pl.ds(pl.multiple_of(g * fdim, 128), fdim)

    own_tok = pltpu.make_async_copy(tok, t.at[y, :, feats(gx)], os.at[0])
    own_bias = pltpu.make_async_copy(bias, bv, os.at[1])
    own_tok.start()
    loop(0, nb, lambda k: wcopy(lax.rem(k + one * half, nb)).start())
    own_bias.start()

    barrier = pltpu.get_barrier_semaphore()

    def hello(dev):
        pl.semaphore_signal(barrier, inc=1, device_id=dev, device_id_type=MESH)

    to_core, to_x, to_q, to_y = (core, y, z), (xp, y, z), (xq, y, z), (gx, oy, z)
    for dev in (to_x, to_q, to_core, to_y):
        hello(dev)

    @pl.when(z > 0)
    def _():
        hello((gx, y, z - 1))

    @pl.when(z < 3)
    def _():
        hello((gx, y, z + 1))

    own_tok.wait()
    pl.semaphore_wait(barrier, jnp.where(end, 5, 6))

    def move(r, lo, n, g, send_sem, recv_sem, dev):
        ref = t.at[r, pl.ds(lo, n), feats(g)]
        return pltpu.make_async_remote_copy(
            src_ref=ref, dst_ref=ref, send_sem=send_sem, recv_sem=recv_sem,
            device_id=dev, device_id_type=MESH)

    np_ = len(pieces)
    halves = ((0, hr), (hr, hr))
    straight = 2
    n0 = pieces[straight][0]
    c0 = move(y, 0, rows_all, gx, ts.at[0], r0.at[0], to_core)
    cq = [move(y, lo, n, gx, ts.at[1], r3.at[q], to_q) if q < straight else None
          for q, (lo, n) in enumerate(pieces)]
    c1 = [move(y, lo, n, gx, ts.at[2], r1.at[q], to_x) for q, (lo, n) in enumerate(pieces)]
    c3 = [move(y, lo, n, xp, ts.at[3], r3.at[q], to_core) if q >= straight else None
          for q, (lo, n) in enumerate(pieces)]
    c2 = [move(y, lo, n, gx, ts.at[4], r2.at[0, h], to_y) for h, (lo, n) in enumerate(halves)]
    c5 = [move(oy, lo, n, gx, ts.at[5], r2.at[1, h], to_x) for h, (lo, n) in enumerate(halves)]
    c4 = [move(oy, lo, n, gx, ts.at[6], r4.at[0, h], to_core) for h, (lo, n) in enumerate(halves)]
    c6 = [move(oy, lo, n, xp, ts.at[7], r4.at[1, h], to_core) for h, (lo, n) in enumerate(halves)]

    for q in range(np_ - 1):
        c1[q].start()
        if q < straight:
            cq[q].start()
        if q == 0:
            c0.start()
            c2[0].start()
    c2[1].start()

    def own_rows(q):
        c1[q].wait_recv()
        if q < straight:
            cq[q].wait_recv()
        else:
            c3[q].start()
            c3[q].wait_recv()
        if q == 0:
            c0.wait_recv()

    def pass_on(h):
        c2[h].wait_recv()
        c5[h].start()
        c4[h].start()
        if h == 0:
            c1[np_ - 1].start()

    def other_rows(h):
        c5[h].wait_recv()
        c6[h].start()
        c4[h].wait_recv()
        c6[h].wait_recv()

    def columns(k):
        return wv[lax.div(k, 2), :, pl.ds(pl.multiple_of(lax.rem(k, 2) * cw, cw), cw)]

    def split(c):
        h, b = lax.div(c, nb), lax.rem(c, nb)
        return pl.ds(pl.multiple_of(h * hr, hr), hr), b

    def dot(r, j, c):
        rows, b = split(c)
        return jnp.dot(t[r, rows], columns(j * nb + b), preferred_element_type=jnp.float32)

    def ycopy(j, c, g):
        at = pl.ds(c, g)
        return pltpu.make_async_remote_copy(
            src_ref=ysend.at[j, at], dst_ref=yrecv.at[j, at], send_sem=yss.at[j],
            recv_sem=yrs.at[j, lax.div(c, group)], device_id=to_y, device_id_type=MESH)

    def zcopy(src, s, m, c, g, dst, sem, dev):
        at = pl.ds(c, g)
        return pltpu.make_async_remote_copy(
            src_ref=src.at[s, at], dst_ref=dst[0].at[dst[1], at], send_sem=zss.at[m],
            recv_sem=sem, device_id=(gx, y, dev), device_id_type=MESH)

    def end_sem(m, c):
        return rms.at[c] if m == 2 else ras.at[m, lax.div(c, group)]

    def from_end(src, s, m, c, g=1):
        return zcopy(src, s, m, c, g, (ra, m), end_sem(m, c), inner)

    def from_mid(s, m, c, dev, g=1):
        return zcopy(zsend, s, s, c, g, (rb, m), rbs.at[m, lax.div(c, group)], dev)

    def grouped(c, wait):
        pl.when(lax.rem(c, group) == 0)(wait)

    def give(j, c):
        ysend[j, c] = encode(dot(oy, j, c))
        ycopy(j, c, 1).start()

    def give_upper():
        other_rows(0)
        loop(0, nb, lambda c: give(first, c))

    def give_lower():
        other_rows(1)
        loop(nb, nc, lambda c: give(first, c))

    def y_wait(j, c):
        grouped(c, lambda: ycopy(j, c, group).wait_recv())

    def a_wait(m, c):
        if m == 2:
            from_end(zsend, m, m, c).wait_recv()
        else:
            grouped(c, lambda: from_end(zsend, m, m, c, group).wait_recv())

    def b_wait(m, c):
        grouped(c, lambda: from_mid(0, m, c, z, group).wait_recv())

    def finish(c, value):
        rows, b = split(c)
        cols = pl.ds(pl.multiple_of(b * cw, cw), cw)
        out[rows, cols] = gelu(value + bv[cols][None, :]).astype(out.dtype)

    def end_send(s, j, c):
        zsend[s, c] = encode(dot(y, j, c))
        from_end(zsend, s, s, c).start()

    def relay(s, j, c):
        y_wait(j, c)
        from_end(yrecv, j, s, c).start()

    def end_last(own, c):
        if own:
            acc[...] = dot(y, zero, c)
        else:
            y_wait(zero, c)
            acc[...] = decode(yrecv[zero, c])
        b_wait(1, c)
        finish(c, acc[...] + decode(rb[1, c]))

    def opening(s):
        for q, (lo, n) in enumerate(pieces[:-1]):
            own_rows(q)
            if s is not None:
                if q == 0:
                    loop(0, half, lambda k: wcopy(one * half + k).wait())
                rows = pl.ds(lo, n)

                def part(b):
                    zsend[s, b, rows] = encode(jnp.dot(
                        t[y, rows], columns(one * nb + b), preferred_element_type=jnp.float32))
                    pltpu.make_async_remote_copy(
                        src_ref=zsend.at[s, b, rows], dst_ref=ra.at[s, b, rows],
                        send_sem=zss.at[s], recv_sem=end_sem(s, b),
                        device_id=(gx, y, inner), device_id_type=MESH).start()

                loop(0, nb, part)
            if q == straight - 1:
                pass_on(0)
        pass_on(1)
        if s is None:
            loop(0, half, lambda k: wcopy(one * half + k).wait())
        loop(0, half, lambda k: wcopy(zero * half + k).wait())
        own_bias.wait()
        give_upper()
        own_rows(np_ - 1)

    ahead = (2 * nc) // 3

    @pl.when(end & own_half)
    def _():
        opening(2)
        loop(nb, ahead, lambda c: end_send(2, one, c))
        give_lower()

        def far(c):
            relay(0, one, c)
            give(zero, c)

        loop(0, nc, far)
        loop(0, nc, lambda c: relay(1, zero, c))
        loop(ahead, nc, lambda c: end_send(2, one, c))
        loop(0, nc, lambda c: end_last(True, c))

    @pl.when(end & other_half)
    def _():
        opening(0)
        loop(nb, nc, lambda c: end_send(0, one, c))
        give_lower()
        loop(0, nc, lambda c: give(zero, c))
        loop(0, nc, lambda c: end_send(1, zero, c))
        loop(0, nc, lambda c: relay(2, one, c))
        loop(0, nc, lambda c: end_last(False, c))

    def partial_of(own, j, c):
        if own:
            return dot(y, j, c)
        y_wait(j, c)
        return decode(yrecv[j, c])

    def up(own, s, j, c):
        acc[...] = partial_of(own, j, c)
        a_wait(s, c)
        zsend[s, c] = encode(acc[...] + decode(ra[s, c]))
        from_mid(s, s, c, far_mid).start()

    def down(own, j, c):
        acc[...] = partial_of(own, j, c)
        b_wait(0, c)
        zsend[2, c] = encode(acc[...] + decode(rb[0, c]))
        from_mid(2, 1, c, near).start()

    def mid_last(own, j, c):
        part = partial_of(own, j, c)
        b_wait(1, c)
        acc[...] = part + decode(rb[1, c])
        a_wait(2, c)
        finish(c, acc[...] + decode(ra[2, c]))

    @pl.when(middle)
    def _():
        opening(None)
        give_lower()
        loop(0, nc, lambda c: give(1 - first, c))

    @pl.when(middle & own_half)
    def _():
        def both(c):
            up(False, 0, one, c)
            down(True, zero, c)

        loop(0, nc, both)

        def mixed(c):
            up(False, 1, zero, c)
            mid_last(True, one, c)

        loop(0, ahead, mixed)
        loop(ahead, nc, lambda c: up(False, 1, zero, c))
        loop(ahead, nc, lambda c: mid_last(True, one, c))

    @pl.when(middle & other_half)
    def _():
        loop(0, nc, lambda c: up(True, 0, one, c))

        def both(c):
            up(True, 1, zero, c)
            down(False, zero, c)

        loop(0, nc, both)
        loop(0, nc, lambda c: mid_last(False, one, c))

    for k, (r, lo, g) in enumerate((
            (y, 0, gx), (y, 0, gx), (y, 0, gx), (y, n0, xp),
            (y, 0, gx), (oy, 0, gx), (oy, 0, gx), (oy, 0, xp))):
        n = n0 if k == 1 else rows_all - lo
        move(r, lo, n, g, ts.at[k], r0.at[0], to_core).wait_send()
    for s in range(3):
        from_end(zsend, s, s, 0, nc).wait_send()
    for j in range(2):
        ycopy(j, 0, nc).wait_send()


def fused(tokens, weight, bias):
    rows, fdim = tokens.shape
    depth, cols = weight.shape
    block = cols // 2
    cw = 256
    hr = rows // 2
    nb = block // cw
    nc = 2 * nb
    group = 2
    cuts = (0, rows // 16, 3 * rows // 16, hr, rows)
    pieces = tuple((a, b - a) for a, b in zip(cuts, cuts[1:]))
    n = len(pieces)
    dma = pltpu.SemaphoreType.DMA
    piece = lambda k: pltpu.VMEM((k, nc, hr, cw), jnp.bfloat16)
    stay = lambda x: pltpu.with_memory_space_constraint(x, pltpu.HBM)
    return pl.pallas_call(
        functools.partial(kernel, nb, hr, cw, group, pieces),
        out_shape=pltpu.VMEM((rows, block), jnp.bfloat16),
        in_specs=[pl.BlockSpec(memory_space=pltpu.HBM)] * 3,
        out_specs=pl.BlockSpec(memory_space=pltpu.VMEM),
        scratch_shapes=[
            pltpu.VMEM((2, rows, depth), jnp.bfloat16),
            pltpu.VMEM((nb, depth, 2 * cw), jnp.bfloat16),
            pltpu.VMEM((block,), jnp.float32),
            pltpu.VMEM((hr, cw), jnp.float32),
            piece(2), piece(2), piece(3), piece(3), piece(2),
            dma((nb,)), dma((2,)), dma((8,)), dma((1,)), dma((n,)), dma((2, 2)), dma((n,)),
            dma((2, 2)), dma((2,)), dma((2, nc // group)), dma((3,)), dma((2, nc // group)),
            dma((nc,)), dma((2, nc // group)),
        ],
        compiler_params=pltpu.CompilerParams(
            has_side_effects=True, collective_id=0, vmem_limit_bytes=52 * 1024 * 1024),
    )(stay(tokens), stay(weight), stay(bias))


def gathered(tokens, weight, bias):
    features = lax.all_gather(tokens, "gx", axis=1, tiled=True)
    columns = lax.all_gather(weight, "gy", axis=1, tiled=True)
    partial_sum = jnp.dot(features, columns, preferred_element_type=jnp.float32)
    owned = lax.psum_scatter(partial_sum, "gz", scatter_dimension=1, tiled=True)
    pre = owned + bias[None, :]
    return jax.nn.gelu(pre, approximate=False).astype(jnp.bfloat16)


def solution(mesh):
    placed = (P("gy", ("gz", "gx")), P("gz", ("gx", "gy")), P(("gx", "gz")))
    sizes = tuple(mesh.shape[a] for a in ("gx", "gy", "gz"))
    per_device = fused if sizes == (4, 2, 4) else gathered
    return jax.shard_map(
        per_device, mesh=mesh, in_specs=placed, out_specs=P("gy", ("gx", "gz")), check_vma=False
    )
```

```python
import functools
import math

import jax
import jax.numpy as jnp
from jax import lax
from jax.experimental import pallas as pl
from jax.experimental.pallas import tpu as pltpu
from jax.sharding import PartitionSpec as P

MESH = pl.DeviceIdType.MESH
POWER = 9
SCALE = 6.0


def encode(p):
    x = p * SCALE
    x2 = x * x
    x4 = x2 * x2
    return ((x4 * x4) * x).astype(jnp.bfloat16)


def decode(code):
    y = code.astype(jnp.float32)
    a = jnp.maximum(jnp.abs(y), 1e-37)
    slope = -(POWER - 1) / POWER * 1.4426950408889634
    return y * jnp.exp2(jnp.log(a) * slope - math.log2(SCALE))


def gelu(v):
    return (v * 0.5) * (1.0 + lax.erf(v * 0.7071067811865476))


def kernel(nb, hr, cw, group, parts, pieces, tok, w, bias, out, t, wv, bv, acc, ysend, yrecv,
           zsend, ra, rb, ws, os, ts, r0, r1, r2, r3, r4, yss, yrs, zss, ras, rms, rbs):
    gx, y, z = (lax.axis_index(a) for a in ("gx", "gy", "gz"))
    rows_all, fdim = tok.shape
    nc = 2 * nb
    core = gx + 1 - 2 * lax.rem(gx, 2)
    xp = lax.rem(gx + 2, 4)
    xq = lax.rem(core + 2, 4)
    oy = 1 - y
    end = (z == 0) | (z == 3)
    middle = jnp.logical_not(end)
    low = z < 2
    own_half = y == z // 2
    other_half = jnp.logical_not(own_half)
    inner = jnp.where(low, 1, 2)
    far_mid = jnp.where(low, 2, 1)
    near = jnp.where(low, 0, 3)
    one = jnp.where(low, 1, 0)
    zero = 1 - one
    first = jnp.where(end, one, y)

    def loop(lo, hi, body):
        def run(c, carry):
            body(c)
            return carry
        lax.fori_loop(lo, hi, run, 0)

    wide = nb // 2

    def wcopy(k):
        cols = pl.ds(pl.multiple_of(k * wide * cw, wide * cw), wide * cw)
        return pltpu.make_async_copy(w.at[:, cols], wv.at[k], ws.at[k])

    def feats(g):
        return pl.ds(pl.multiple_of(g * fdim, 128), fdim)

    own_tok = pltpu.make_async_copy(tok, t.at[y, :, feats(gx)], os.at[0])
    own_bias = pltpu.make_async_copy(bias, bv, os.at[1])
    own_tok.start()
    loop(0, 4, lambda k: wcopy(lax.rem(k + one * 2, 4)).start())
    own_bias.start()

    barrier = pltpu.get_barrier_semaphore()

    def hello(dev):
        pl.semaphore_signal(barrier, inc=1, device_id=dev, device_id_type=MESH)

    to_core, to_x, to_q, to_y = (core, y, z), (xp, y, z), (xq, y, z), (gx, oy, z)
    for dev in (to_x, to_q, to_core, to_y):
        hello(dev)

    @pl.when(z > 0)
    def _():
        hello((gx, y, z - 1))

    @pl.when(z < 3)
    def _():
        hello((gx, y, z + 1))

    own_tok.wait()
    pl.semaphore_wait(barrier, jnp.where(end, 5, 6))

    def move(r, lo, n, g, recv_sem, dev, width=1):
        ref = t.at[r, pl.ds(lo, n), pl.ds(pl.multiple_of(g * fdim, 128), width * fdim)]
        return pltpu.make_async_remote_copy(
            src_ref=ref, dst_ref=ref, send_sem=ts.at[0], recv_sem=recv_sem,
            device_id=dev, device_id_type=MESH)

    npiece = len(pieces)
    halves = ((0, hr), (hr, hr))
    straight = 2
    cq = [move(y, lo, n, gx, r1.at[q], to_q) for q, (lo, n) in enumerate(pieces[:straight])]
    c0 = [move(y, lo, n, gx, r1.at[q] if q < straight else r3.at[q - straight], to_core)
          for q, (lo, n) in enumerate(pieces)]
    c1 = [move(y, lo, n, gx, r1.at[q], to_x) for q, (lo, n) in enumerate(pieces)]
    c3 = [move(y, lo, n, xp, r3.at[q], to_core) for q, (lo, n) in enumerate(pieces[straight:])]
    c2 = [move(y, lo, n, gx, r2.at[0, h], to_y) for h, (lo, n) in enumerate(halves)]
    c5 = [move(oy, lo, n, gx, r2.at[1, h], to_x) for h, (lo, n) in enumerate(halves)]
    c4 = [move(oy, lo, n, gx, r4.at[h], to_core) for h, (lo, n) in enumerate(halves)]
    c6 = [move(oy, lo, n, xp, r4.at[h], to_core) for h, (lo, n) in enumerate(halves)]

    even = lax.rem(gx, 2) == 0

    def go(q):
        @pl.when(even)
        def _():
            c1[q].start()
            cq[q].start()

        @pl.when(jnp.logical_not(even))
        def _():
            cq[q].start()
            c1[q].start()

    for q in range(npiece - 1):
        if q < straight:
            go(q)
        else:
            c1[q].start()
        c0[q].start()
        if q == 0:
            c2[0].start()
    c0[npiece - 1].start()
    c2[1].start()

    def own_rows(q):
        lo, n = pieces[q]
        if q < straight:
            move(y, lo, n, 0, r1.at[q], to_x, 3).wait_recv()
        else:
            c1[q].wait_recv()
            c3[q - straight].start()
            move(y, lo, n, 0, r3.at[q - straight], to_core, 2).wait_recv()

    def pass_on(h):
        c2[h].wait_recv()
        c5[h].start()
        c4[h].start()
        if h == 0:
            c1[npiece - 1].start()

    def other_rows(h):
        lo, n = halves[h]
        c5[h].wait_recv()
        c6[h].start()
        move(oy, lo, n, 0, r4.at[h], to_core, 2).wait_recv()

    def columns(k):
        return wv[lax.div(k, wide), :, pl.ds(pl.multiple_of(lax.rem(k, wide) * cw, cw), cw)]

    def split(c):
        h, b = lax.div(c, nb), lax.rem(c, nb)
        return pl.ds(pl.multiple_of(h * hr, hr), hr), b

    def dot(r, j, c):
        rows, b = split(c)
        return jnp.dot(t[r, rows], columns(j * nb + b), preferred_element_type=jnp.float32)

    def ycopy(j, c, g):
        at = pl.ds(c, g)
        return pltpu.make_async_remote_copy(
            src_ref=ysend.at[j, at], dst_ref=yrecv.at[j, at], send_sem=yss.at[0],
            recv_sem=yrs.at[j, lax.div(c, group)], device_id=to_y, device_id_type=MESH)

    def zcopy(src, s, m, c, g, dst, sem, dev):
        at = pl.ds(c, g)
        return pltpu.make_async_remote_copy(
            src_ref=src.at[s, at], dst_ref=dst[0].at[dst[1], at], send_sem=zss.at[0],
            recv_sem=sem, device_id=(gx, y, dev), device_id_type=MESH)

    def end_sem(m, c):
        return rms.at[lax.div(c, group)] if m == 2 else ras.at[m, lax.div(c, group)]

    def from_end(src, s, m, c, g=1):
        return zcopy(src, s, m, c, g, (ra, m), end_sem(m, c), inner)

    def from_mid(s, m, c, dev, g=1):
        return zcopy(zsend, s, s, c, g, (rb, m), rbs.at[m, lax.div(c, group)], dev)

    def grouped(c, wait):
        if isinstance(c, int):
            if c % group == 0:
                wait()
        else:
            pl.when(lax.rem(c, group) == 0)(wait)

    def give(j, c):
        ysend[j, c] = encode(dot(oy, j, c))
        ycopy(j, c, 1).start()

    def give_upper():
        other_rows(0)
        loop(0, nb, lambda c: give(first, c))

    def give_lower():
        other_rows(1)
        loop(nb, nc, lambda c: give(first, c))

    def y_wait(j, c):
        grouped(c, lambda: ycopy(j, c, group).wait_recv())

    def a_wait(m, c):
        g = 1 if isinstance(c, int) else group
        grouped(c, lambda: from_end(zsend, m, m, c, g).wait_recv())

    def b_wait(m, c):
        grouped(c, lambda: from_mid(0, m, c, z, group).wait_recv())

    def finish(c, value):
        rows, b = split(c)
        cols = pl.ds(pl.multiple_of(b * cw, cw), cw)
        out[rows, cols] = gelu(value + bv[cols][None, :]).astype(out.dtype)

    def in_parts(src, s):
        for k in range(parts):
            rows = pl.ds(k * (hr // parts), hr // parts)
            yield rows, pltpu.make_async_remote_copy(
                src_ref=src.at[s, nc - 1, rows], dst_ref=ra.at[2, nc - 1, rows],
                send_sem=zss.at[0], recv_sem=rms.at[nc // group + k],
                device_id=(gx, y, inner), device_id_type=MESH)

    def end_send(s, j, c, g=1):
        for k in range(g):
            zsend[s, c + k] = encode(dot(y, j, c + k))
        from_end(zsend, s, s, c, g).start()

    def relay(s, j, c, g=1):
        y_wait(j, c)
        from_end(yrecv, j, s, c, g).start()

    def pairs(lo, hi, body):
        loop(lo // group, hi // group, lambda k: body(k * group))

    def end_last(own, c):
        if own:
            acc[...] = dot(y, zero, c)
        else:
            y_wait(zero, c)
            acc[...] = decode(yrecv[zero, c])
        b_wait(1, c)
        finish(c, acc[...] + decode(rb[1, c]))

    def opening(s):
        for q, (lo, n) in enumerate(pieces[:-1]):
            own_rows(q)
            if s is not None:
                if q == 0:
                    loop(0, 2, lambda k: wcopy(one * 2 + k).wait())
                rows = pl.ds(lo, n)

                def part(b):
                    zsend[s, b, rows] = encode(jnp.dot(
                        t[y, rows], columns(one * nb + b), preferred_element_type=jnp.float32))
                    pltpu.make_async_remote_copy(
                        src_ref=zsend.at[s, b, rows], dst_ref=ra.at[s, b, rows],
                        send_sem=zss.at[0], recv_sem=end_sem(s, b),
                        device_id=(gx, y, inner), device_id_type=MESH).start()

                loop(0, nb, part)
            if q == straight - 1:
                pass_on(0)
        pass_on(1)
        if s is None:
            loop(0, 2, lambda k: wcopy(one * 2 + k).wait())
        loop(0, 2, lambda k: wcopy(zero * 2 + k).wait())
        own_bias.wait()
        give_upper()
        own_rows(npiece - 1)

    ahead = (2 * nc) // 3

    @pl.when(end & own_half)
    def _():
        opening(2)
        pairs(nb, ahead, lambda c: end_send(2, one, c, group))
        give_lower()

        def far(c):
            relay(0, one, c, group)
            for k in range(group):
                give(zero, c + k)

        pairs(0, nc, far)
        pairs(0, nc, lambda c: relay(1, zero, c, group))
        pairs(ahead, nc - group, lambda c: end_send(2, one, c, group))
        end_send(2, one, nc - 2)
        zsend[2, nc - 1] = encode(dot(y, one, nc - 1))
        for _, copy in in_parts(zsend, 2):
            copy.start()
        loop(0, nc, lambda c: end_last(True, c))

    @pl.when(end & other_half)
    def _():
        opening(0)
        pairs(nb, nc, lambda c: end_send(0, one, c, group))
        give_lower()
        loop(0, nc, lambda c: give(zero, c))
        pairs(0, nc, lambda c: end_send(1, zero, c, group))
        pairs(0, nc - group, lambda c: relay(2, one, c, group))
        relay(2, one, nc - 2)
        for _, copy in in_parts(yrecv, one):
            copy.start()
        loop(0, nc, lambda c: end_last(False, c))

    def partial_of(own, j, c):
        if own:
            return dot(y, j, c)
        y_wait(j, c)
        return decode(yrecv[j, c])

    def up(own, s, j, c):
        acc[...] = partial_of(own, j, c)
        a_wait(s, c)
        zsend[s, c] = encode(acc[...] + decode(ra[s, c]))
        from_mid(s, s, c, far_mid).start()

    def down(own, j, c):
        acc[...] = partial_of(own, j, c)
        b_wait(0, c)
        zsend[2, c] = encode(acc[...] + decode(rb[0, c]))
        from_mid(2, 1, c, near).start()

    def mid_final(own, j):
        c = nc - 1
        part = partial_of(own, j, c)
        b_wait(1, c)
        lo, b = (nc - 1) // nb * hr, (nc - 1) % nb
        cols = pl.ds(b * cw, cw)
        acc[...] = part + decode(rb[1, c]) + bv[cols][None, :]
        for rows, copy in in_parts(zsend, 2):
            copy.wait_recv()
            v = acc[rows] + decode(ra[2, c, rows])
            out[pl.ds(lo + rows.start, hr // parts), cols] = gelu(v).astype(out.dtype)

    def mid_last(own, j, c):
        part = partial_of(own, j, c)
        b_wait(1, c)
        acc[...] = part + decode(rb[1, c])
        a_wait(2, c)
        finish(c, acc[...] + decode(ra[2, c]))

    @pl.when(middle)
    def _():
        opening(None)
        give_lower()
        loop(0, nc, lambda c: give(1 - first, c))

    @pl.when(middle & own_half)
    def _():
        def both(c):
            up(False, 0, one, c)
            down(True, zero, c)

        loop(0, nc, both)

        def mixed(c):
            up(False, 1, zero, c)
            mid_last(True, one, c)

        loop(0, ahead, mixed)
        loop(ahead, nc, lambda c: up(False, 1, zero, c))
        loop(ahead, nc - 2, lambda c: mid_last(True, one, c))
        mid_last(True, one, nc - 2)
        mid_final(True, one)

    @pl.when(middle & other_half)
    def _():
        loop(0, nc, lambda c: up(True, 0, one, c))

        def both(c):
            up(True, 1, zero, c)
            down(False, zero, c)

        loop(0, nc, both)
        loop(0, nc - 2, lambda c: mid_last(False, one, c))
        mid_last(False, one, nc - 2)
        mid_final(False, one)

    def gone(src, dst, sem):
        pltpu.make_async_remote_copy(
            src_ref=src, dst_ref=dst, send_sem=sem.at[0], recv_sem=r0.at[0],
            device_id=to_core, device_id_type=MESH).wait_send()

    most = t.at[:, pl.ds(0, 7 * rows_all // 8)]
    gone(most, most, ts)
    gone(ysend, yrecv, yss)
    gone(zsend, ra, zss)


def fused(tokens, weight, bias):
    rows, fdim = tokens.shape
    depth, cols = weight.shape
    block = cols // 2
    cw = 256
    hr = rows // 2
    nb = block // cw
    nc = 2 * nb
    group = 2
    parts = 4
    cuts = (0, rows // 16, 3 * rows // 16, hr, rows)
    pieces = tuple((a, b - a) for a, b in zip(cuts, cuts[1:]))
    n = len(pieces)
    dma = pltpu.SemaphoreType.DMA
    piece = lambda k: pltpu.VMEM((k, nc, hr, cw), jnp.bfloat16)
    stay = lambda x: pltpu.with_memory_space_constraint(x, pltpu.HBM)
    return pl.pallas_call(
        functools.partial(kernel, nb, hr, cw, group, parts, pieces),
        out_shape=pltpu.VMEM((rows, block), jnp.bfloat16),
        in_specs=[pl.BlockSpec(memory_space=pltpu.HBM)] * 3,
        out_specs=pl.BlockSpec(memory_space=pltpu.VMEM),
        scratch_shapes=[
            pltpu.VMEM((2, rows, depth), jnp.bfloat16),
            pltpu.VMEM((4, depth, nb // 2 * cw), jnp.bfloat16),
            pltpu.VMEM((block,), jnp.float32),
            pltpu.VMEM((hr, cw), jnp.float32),
            piece(2), piece(2), piece(3), piece(3), piece(2),
            dma((4,)), dma((2,)), dma((1,)), dma((1,)), dma((n,)), dma((2, 2)), dma((n - 2,)),
            dma((2,)), dma((1,)), dma((2, nc // group)), dma((1,)), dma((2, nc // group)),
            dma((nc // group + parts,)), dma((2, nc // group)),
        ],
        compiler_params=pltpu.CompilerParams(
            has_side_effects=True, collective_id=0, vmem_limit_bytes=52 * 1024 * 1024),
    )(stay(tokens), stay(weight), stay(bias))


def gathered(tokens, weight, bias):
    features = lax.all_gather(tokens, "gx", axis=1, tiled=True)
    columns = lax.all_gather(weight, "gy", axis=1, tiled=True)
    partial_sum = jnp.dot(features, columns, preferred_element_type=jnp.float32)
    owned = lax.psum_scatter(partial_sum, "gz", scatter_dimension=1, tiled=True)
    pre = owned + bias[None, :]
    return jax.nn.gelu(pre, approximate=False).astype(jnp.bfloat16)


def solution(mesh):
    placed = (P("gy", ("gz", "gx")), P("gz", ("gx", "gy")), P(("gx", "gz")))
    sizes = tuple(mesh.shape[a] for a in ("gx", "gy", "gz"))
    per_device = fused if sizes == (4, 2, 4) else gathered
    return jax.shard_map(
        per_device, mesh=mesh, in_specs=placed, out_specs=P("gy", ("gx", "gz")), check_vma=False
    )
```

```python
import functools
import math

import jax
import jax.numpy as jnp
from jax import lax
from jax.experimental import pallas as pl
from jax.experimental.pallas import tpu as pltpu
from jax.sharding import PartitionSpec as P

MESH = pl.DeviceIdType.MESH
POWER = 9
SCALE = 6.0


def encode(p):
    x = p * SCALE
    x2 = x * x
    x4 = x2 * x2
    return ((x4 * x4) * x).astype(jnp.bfloat16)


def decode(code):
    y = code.astype(jnp.float32)
    a = jnp.maximum(jnp.abs(y), 1e-37)
    slope = -(POWER - 1) / POWER * 1.4426950408889634
    return y * jnp.exp2(jnp.log(a) * slope - math.log2(SCALE))


def gelu(v):
    return (v * 0.5) * (1.0 + lax.erf(v * 0.7071067811865476))


def kernel(nb, hr, cw, group, parts, pieces, tok, w, bias, out, t, wv, bv, acc, ysend, yrecv,
           zsend, ra, rb, ws, os, ts, r0, r1, r2, r3, r4, yss, yrs, zss, ras, rms, rbs):
    gx, y, z = (lax.axis_index(a) for a in ("gx", "gy", "gz"))
    rows_all, fdim = tok.shape
    nc = 2 * nb
    core = gx + 1 - 2 * lax.rem(gx, 2)
    xp = lax.rem(gx + 2, 4)
    xq = lax.rem(core + 2, 4)
    oy = 1 - y
    end = (z == 0) | (z == 3)
    middle = jnp.logical_not(end)
    low = z < 2
    own_half = y == z // 2
    other_half = jnp.logical_not(own_half)
    inner = jnp.where(low, 1, 2)
    far_mid = jnp.where(low, 2, 1)
    near = jnp.where(low, 0, 3)
    one = jnp.where(low, 1, 0)
    zero = 1 - one
    first = jnp.where(end, one, y)

    def loop(lo, hi, body):
        def run(c, carry):
            body(c)
            return carry
        lax.fori_loop(lo, hi, run, 0)

    wide = group
    nw = nb // group

    def wcopy(k):
        cols = pl.ds(pl.multiple_of(k * wide * cw, wide * cw), wide * cw)
        return pltpu.make_async_copy(w.at[:, cols], wv.at[k], ws.at[k])

    def feats(g):
        return pl.ds(pl.multiple_of(g * fdim, 128), fdim)

    own_tok = pltpu.make_async_copy(tok, t.at[y, :, feats(gx)], os.at[0])
    own_bias = pltpu.make_async_copy(bias, bv, os.at[1])
    own_tok.start()
    loop(0, 2 * nw, lambda k: wcopy(lax.rem(k + one * nw, 2 * nw)).start())
    own_bias.start()

    barrier = pltpu.get_barrier_semaphore()

    def hello(dev):
        pl.semaphore_signal(barrier, inc=1, device_id=dev, device_id_type=MESH)

    to_core, to_x, to_q, to_y = (core, y, z), (xp, y, z), (xq, y, z), (gx, oy, z)
    for dev in (to_x, to_q, to_core, to_y):
        hello(dev)

    @pl.when(z > 0)
    def _():
        hello((gx, y, z - 1))

    @pl.when(z < 3)
    def _():
        hello((gx, y, z + 1))

    own_tok.wait()
    pl.semaphore_wait(barrier, jnp.where(end, 5, 6))

    def move(r, lo, n, g, recv_sem, dev, width=1):
        ref = t.at[r, pl.ds(lo, n), pl.ds(pl.multiple_of(g * fdim, 128), width * fdim)]
        return pltpu.make_async_remote_copy(
            src_ref=ref, dst_ref=ref, send_sem=ts.at[0], recv_sem=recv_sem,
            device_id=dev, device_id_type=MESH)

    npiece = len(pieces)
    halves = ((0, hr), (hr, hr))
    straight = 2
    cq = [move(y, lo, n, gx, r1.at[q], to_q) for q, (lo, n) in enumerate(pieces[:straight])]
    c0 = [move(y, lo, n, gx, r1.at[q] if q < straight else r3.at[q - straight], to_core)
          for q, (lo, n) in enumerate(pieces)]
    c1 = [move(y, lo, n, gx, r1.at[q], to_x) for q, (lo, n) in enumerate(pieces)]
    c3 = [move(y, lo, n, xp, r3.at[q], to_core) for q, (lo, n) in enumerate(pieces[straight:])]
    c2 = [move(y, lo, n, gx, r2.at[0, h], to_y) for h, (lo, n) in enumerate(halves)]
    c5 = [move(oy, lo, n, gx, r2.at[1, h], to_x) for h, (lo, n) in enumerate(halves)]
    c4 = [move(oy, lo, n, gx, r4.at[h], to_core) for h, (lo, n) in enumerate(halves)]
    c6 = [move(oy, lo, n, xp, r4.at[h], to_core) for h, (lo, n) in enumerate(halves)]

    even = lax.rem(gx, 2) == 0

    def go(q):
        @pl.when(even)
        def _():
            c1[q].start()
            cq[q].start()

        @pl.when(jnp.logical_not(even))
        def _():
            cq[q].start()
            c1[q].start()

    for q in range(npiece - 1):
        if q < straight:
            go(q)
        else:
            c1[q].start()
        c0[q].start()
        if q == 0:
            c2[0].start()
    c0[npiece - 1].start()
    c2[1].start()

    def own_rows(q):
        lo, n = pieces[q]
        if q < straight:
            move(y, lo, n, 0, r1.at[q], to_x, 3).wait_recv()
        else:
            c1[q].wait_recv()
            c3[q - straight].start()
            move(y, lo, n, 0, r3.at[q - straight], to_core, 2).wait_recv()

    def pass_on(h):
        c2[h].wait_recv()
        c5[h].start()
        c4[h].start()
        if h == 0:
            c1[npiece - 1].start()

    def other_rows(h):
        lo, n = halves[h]
        c5[h].wait_recv()
        c6[h].start()
        move(oy, lo, n, 0, r4.at[h], to_core, 2).wait_recv()

    def columns(k):
        return wv[lax.div(k, wide), :, pl.ds(pl.multiple_of(lax.rem(k, wide) * cw, cw), cw)]

    def split(c):
        h, b = lax.div(c, nb), lax.rem(c, nb)
        return pl.ds(pl.multiple_of(h * hr, hr), hr), b

    def dot(r, j, c):
        rows, b = split(c)
        return jnp.dot(t[r, rows], columns(j * nb + b), preferred_element_type=jnp.float32)

    def ycopy(j, c, g):
        at = pl.ds(c, g)
        return pltpu.make_async_remote_copy(
            src_ref=ysend.at[j, at], dst_ref=yrecv.at[j, at], send_sem=yss.at[0],
            recv_sem=yrs.at[j, lax.div(c, group)], device_id=to_y, device_id_type=MESH)

    def zcopy(src, s, m, c, g, dst, sem, dev):
        at = pl.ds(c, g)
        return pltpu.make_async_remote_copy(
            src_ref=src.at[s, at], dst_ref=dst[0].at[dst[1], at], send_sem=zss.at[0],
            recv_sem=sem, device_id=(gx, y, dev), device_id_type=MESH)

    def end_sem(m, c):
        return rms.at[lax.div(c, group)] if m == 2 else ras.at[m, lax.div(c, group)]

    def from_end(src, s, m, c, g=1):
        return zcopy(src, s, m, c, g, (ra, m), end_sem(m, c), inner)

    def from_mid(s, m, c, dev, g=1):
        return zcopy(zsend, s, s, c, g, (rb, m), rbs.at[m, lax.div(c, group)], dev)

    def grouped(c, wait):
        if isinstance(c, int):
            if c % group == 0:
                wait()
        else:
            pl.when(lax.rem(c, group) == 0)(wait)

    def give(j, c):
        ysend[j, c] = encode(dot(oy, j, c))
        ycopy(j, c, 1).start()

    def give_upper():
        other_rows(0)
        loop(0, nb, lambda c: give(first, c))

    def give_lower():
        other_rows(1)
        loop(nb, nc, lambda c: give(first, c))

    def y_wait(j, c):
        grouped(c, lambda: ycopy(j, c, group).wait_recv())

    def a_wait(m, c):
        g = 1 if isinstance(c, int) else group
        grouped(c, lambda: from_end(zsend, m, m, c, g).wait_recv())

    def b_wait(m, c):
        grouped(c, lambda: from_mid(0, m, c, z, group).wait_recv())

    def finish(c, value):
        rows, b = split(c)
        cols = pl.ds(pl.multiple_of(b * cw, cw), cw)
        out[rows, cols] = gelu(value + bv[cols][None, :]).astype(out.dtype)

    def in_parts(src, s):
        for k in range(parts):
            rows = pl.ds(k * (hr // parts), hr // parts)
            yield rows, pltpu.make_async_remote_copy(
                src_ref=src.at[s, nc - 1, rows], dst_ref=ra.at[2, nc - 1, rows],
                send_sem=zss.at[0], recv_sem=rms.at[nc // group + k],
                device_id=(gx, y, inner), device_id_type=MESH)

    def end_send(s, j, c, g=1):
        for k in range(g):
            zsend[s, c + k] = encode(dot(y, j, c + k))
        from_end(zsend, s, s, c, g).start()

    def relay(s, j, c, g=1):
        y_wait(j, c)
        from_end(yrecv, j, s, c, g).start()

    def pairs(lo, hi, body):
        loop(lo // group, hi // group, lambda k: body(k * group))

    def end_last(own, c):
        if own:
            acc[...] = dot(y, zero, c)
        else:
            y_wait(zero, c)
            acc[...] = decode(yrecv[zero, c])
        b_wait(1, c)
        finish(c, acc[...] + decode(rb[1, c]))

    def opening(s):
        for q, (lo, n) in enumerate(pieces[:-1]):
            own_rows(q)
            if s is not None:
                if q == 0:
                    loop(0, nw, lambda k: wcopy(one * nw + k).wait())
                rows = pl.ds(lo, n)

                def part(k):
                    got = encode(jnp.dot(
                        t[y, rows], wv[one * nw + k], preferred_element_type=jnp.float32))
                    for i in range(wide):
                        zsend[s, k * wide + i, rows] = got[:, i * cw:(i + 1) * cw]
                    at = pl.ds(k * wide, wide)
                    pltpu.make_async_remote_copy(
                        src_ref=zsend.at[s, at, rows], dst_ref=ra.at[s, at, rows],
                        send_sem=zss.at[0], recv_sem=end_sem(s, k * wide),
                        device_id=(gx, y, inner), device_id_type=MESH).start()

                for k in range(nw):
                    part(k)
            if q == straight - 1:
                pass_on(0)
        pass_on(1)
        if s is None:
            loop(0, nw, lambda k: wcopy(one * nw + k).wait())
        loop(0, nw, lambda k: wcopy(zero * nw + k).wait())
        own_bias.wait()
        give_upper()
        own_rows(npiece - 1)

    ahead = (2 * nc) // 3

    @pl.when(end & own_half)
    def _():
        opening(2)
        pairs(nb, ahead, lambda c: end_send(2, one, c, group))
        give_lower()

        def far(c):
            relay(0, one, c, group)
            for k in range(group):
                give(zero, c + k)

        pairs(0, nc, far)
        pairs(0, nc, lambda c: relay(1, zero, c, group))
        pairs(ahead, nc - group, lambda c: end_send(2, one, c, group))
        end_send(2, one, nc - 2)
        zsend[2, nc - 1] = encode(dot(y, one, nc - 1))
        for _, copy in in_parts(zsend, 2):
            copy.start()
        loop(0, nc, lambda c: end_last(True, c))

    @pl.when(end & other_half)
    def _():
        opening(0)
        pairs(nb, nc, lambda c: end_send(0, one, c, group))
        give_lower()
        loop(0, nc, lambda c: give(zero, c))
        pairs(0, nc, lambda c: end_send(1, zero, c, group))
        pairs(0, nc - group, lambda c: relay(2, one, c, group))
        relay(2, one, nc - 2)
        for _, copy in in_parts(yrecv, one):
            copy.start()
        loop(0, nc, lambda c: end_last(False, c))

    def partial_of(own, j, c):
        if own:
            return dot(y, j, c)
        y_wait(j, c)
        return decode(yrecv[j, c])

    def up(own, s, j, c):
        acc[...] = partial_of(own, j, c)
        a_wait(s, c)
        zsend[s, c] = encode(acc[...] + decode(ra[s, c]))
        from_mid(s, s, c, far_mid).start()

    def down(own, j, c):
        acc[...] = partial_of(own, j, c)
        b_wait(0, c)
        zsend[2, c] = encode(acc[...] + decode(rb[0, c]))
        from_mid(2, 1, c, near).start()

    def mid_final(own, j):
        c = nc - 1
        part = partial_of(own, j, c)
        b_wait(1, c)
        lo, b = (nc - 1) // nb * hr, (nc - 1) % nb
        cols = pl.ds(b * cw, cw)
        acc[...] = part + decode(rb[1, c]) + bv[cols][None, :]
        for rows, copy in in_parts(zsend, 2):
            copy.wait_recv()
            v = acc[rows] + decode(ra[2, c, rows])
            out[pl.ds(lo + rows.start, hr // parts), cols] = gelu(v).astype(out.dtype)

    def mid_last(own, j, c):
        part = partial_of(own, j, c)
        b_wait(1, c)
        acc[...] = part + decode(rb[1, c])
        a_wait(2, c)
        finish(c, acc[...] + decode(ra[2, c]))

    @pl.when(middle)
    def _():
        opening(None)
        give_lower()
        loop(0, nc, lambda c: give(1 - first, c))

    @pl.when(middle & own_half)
    def _():
        def both(c):
            up(False, 0, one, c)
            down(True, zero, c)

        loop(0, nc, both)

        def mixed(c):
            up(False, 1, zero, c)
            mid_last(True, one, c)

        loop(0, ahead, mixed)
        loop(ahead, nc, lambda c: up(False, 1, zero, c))
        loop(ahead, nc - 2, lambda c: mid_last(True, one, c))
        mid_last(True, one, nc - 2)
        mid_final(True, one)

    @pl.when(middle & other_half)
    def _():
        loop(0, nc, lambda c: up(True, 0, one, c))

        def both(c):
            up(True, 1, zero, c)
            down(False, zero, c)

        loop(0, nc, both)
        loop(0, nc - 2, lambda c: mid_last(False, one, c))
        mid_last(False, one, nc - 2)
        mid_final(False, one)

    def gone(src, dst, sem):
        pltpu.make_async_remote_copy(
            src_ref=src, dst_ref=dst, send_sem=sem.at[0], recv_sem=r0.at[0],
            device_id=to_core, device_id_type=MESH).wait_send()

    most = t.at[:, pl.ds(0, 7 * rows_all // 8)]
    gone(most, most, ts)
    gone(ysend, yrecv, yss)
    gone(zsend, ra, zss)


def fused(tokens, weight, bias):
    rows, fdim = tokens.shape
    depth, cols = weight.shape
    block = cols // 2
    cw = 256
    hr = rows // 2
    nb = block // cw
    nc = 2 * nb
    group = 2
    parts = 4
    cuts = (0, rows // 32, rows // 8, rows // 4, hr, rows)
    pieces = tuple((a, b - a) for a, b in zip(cuts, cuts[1:]))
    n = len(pieces)
    dma = pltpu.SemaphoreType.DMA
    piece = lambda k: pltpu.VMEM((k, nc, hr, cw), jnp.bfloat16)
    stay = lambda x: pltpu.with_memory_space_constraint(x, pltpu.HBM)
    return pl.pallas_call(
        functools.partial(kernel, nb, hr, cw, group, parts, pieces),
        out_shape=pltpu.VMEM((rows, block), jnp.bfloat16),
        in_specs=[pl.BlockSpec(memory_space=pltpu.HBM)] * 3,
        out_specs=pl.BlockSpec(memory_space=pltpu.VMEM),
        scratch_shapes=[
            pltpu.VMEM((2, rows, depth), jnp.bfloat16),
            pltpu.VMEM((nc // group, depth, group * cw), jnp.bfloat16),
            pltpu.VMEM((block,), jnp.float32),
            pltpu.VMEM((hr, cw), jnp.float32),
            piece(2), piece(2), piece(3), piece(3), piece(2),
            dma((nc // group,)), dma((2,)), dma((1,)), dma((1,)), dma((n,)), dma((2, 2)), dma((n - 2,)),
            dma((2,)), dma((1,)), dma((2, nc // group)), dma((1,)), dma((2, nc // group)),
            dma((nc // group + parts,)), dma((2, nc // group)),
        ],
        compiler_params=pltpu.CompilerParams(
            has_side_effects=True, collective_id=0, vmem_limit_bytes=52 * 1024 * 1024),
    )(stay(tokens), stay(weight), stay(bias))


def gathered(tokens, weight, bias):
    features = lax.all_gather(tokens, "gx", axis=1, tiled=True)
    columns = lax.all_gather(weight, "gy", axis=1, tiled=True)
    partial_sum = jnp.dot(features, columns, preferred_element_type=jnp.float32)
    owned = lax.psum_scatter(partial_sum, "gz", scatter_dimension=1, tiled=True)
    pre = owned + bias[None, :]
    return jax.nn.gelu(pre, approximate=False).astype(jnp.bfloat16)


def solution(mesh):
    placed = (P("gy", ("gz", "gx")), P("gz", ("gx", "gy")), P(("gx", "gz")))
    sizes = tuple(mesh.shape[a] for a in ("gx", "gy", "gz"))
    per_device = fused if sizes == (4, 2, 4) else gathered
    return jax.shard_map(
        per_device, mesh=mesh, in_specs=placed, out_specs=P("gy", ("gx", "gz")), check_vma=False
    )
```
